32 devices in a mesh: grp: 4 (over z), ep: 8 (over y, x, core).
Axes of the slice: x: 2, y: 2, z: 4, core: 2. Of those that a mesh axis runs over, the one named last changes fastest.
Arguments:
- hidden: bfloat16 [4, 8, 32, 1024], P('grp', 'ep'), may hold values from -6 to 6
- down_weight: bfloat16 [8, 1024, 4096], P('ep'), may hold values from -0.1875 to 0.1875
- slot_gate: float32 [4, 8, 32], P('grp', 'ep'), may hold values from 0.02 to 0.6
- slot_owner: int32 [4, 8, 32], P('grp', 'ep'), may hold values from 0 to 3
- slot_row: int32 [4, 8, 32], P('grp', 'ep'), may hold values from 0 to 31
- block_count: int32 [4, 8, 8], P('grp', 'ep'), may hold values from 0 to 4, as said below
Outputs:
- mixed: bfloat16 [1024, 4096], P(('grp', 'ep'))
The draws below stay inside these ranges and needn't reach their ends.
Inputs may be any that keep to these rules, and one draw needn't show every extreme that they name: `block_count`: every device's expert has at least one block with all 4 slots live.
All inputs are finite; a program needn't handle non-finite values.
Results may differ from the reference program's by a relative error of at most 0.009.
Values may be sent and summed in bfloat16 or wider, within the bound.
A program may use at most 64 MiB of HBM per device.

```python
import math
import jax
import jax.numpy as jnp
from jax import lax

D = 4096
FFW = 1024
TOK_DEV = 32
SEND = 4
EXPERTS = 8
GROUPS = 4
COLUMNS = 8
SLOTS = 32
TOKENS = 1024
N_EP = 8


def draw_block_count(key, part):
    base = jax.random.randint(jax.random.fold_in(key, 11), (GROUPS, EXPERTS, COLUMNS), 0, SEND + 1)
    chosen = jax.random.randint(jax.random.fold_in(key, 12), (GROUPS, EXPERTS, 1), 0, COLUMNS)
    places = jnp.arange(COLUMNS).astype(jnp.int32)[None, None, :]
    return jnp.where(places == chosen, SEND, base).astype(jnp.int32)


def place_ends(result, stream_key, smallest, top_value):
    index_at = [jax.random.randint(jax.random.fold_in(stream_key, axis), (), 0, length) for axis, length in enumerate(result.shape)]
    widest = result.shape.index(max(result.shape))
    neighbour = index_at[:widest] + [(index_at[widest] + 1) % result.shape[widest]] + index_at[widest + 1:]
    return result.at[tuple(index_at)].set(smallest).at[tuple(neighbour)].set(top_value)


def shard_levels(rng, extent, pieces, smallest, high):
    def one(dim, shards_of):
        draws = jax.random.uniform(jax.random.fold_in(jax.random.fold_in(rng, 6), dim), (shards_of,), jnp.float32, smallest / len(pieces), high / len(pieces))
        return jnp.repeat(jnp.exp(draws), extent[dim] // shards_of).reshape((-1,) + (1,) * (len(extent) - dim - 1))

    gain = one(*pieces[0])
    for cut in pieces[1:]:
        gain = gain * one(*cut)
    return gain


def normal_values(rng, extent, width, bound, pieces=(), dtype=jnp.bfloat16):
    factor_of = shard_levels(rng, extent, pieces, -0.22, 0.18) if pieces else 1.0
    result = jax.random.normal(rng, extent, jnp.float32) * width * factor_of
    return jnp.minimum(jnp.maximum(result, -bound), bound).astype(dtype)


def setup_inputs(seed: int = 0) -> dict:
    key_of = jax.random.split(jax.random.key(seed), 7)
    hidden = normal_values(key_of[0], (GROUPS, EXPERTS, SLOTS, FFW), 1.0, 6.0, ((0, 4), (1, 8)))
    down_weight = normal_values(key_of[1], (EXPERTS, FFW, D), FFW ** -0.5, 0.1875, ((0, 8),))
    slot_gate = jnp.clip(jnp.exp(math.log(0.6) - 3.4011974 * jax.random.uniform(key_of[2], (GROUPS, EXPERTS, SLOTS), jnp.float32) ** shard_levels(key_of[2], (GROUPS, EXPERTS, SLOTS), ((0, 4), (1, 8)), -0.2, 0.2)), 0.02, 0.6)
    slot_owner = place_ends(jax.random.randint(key_of[3], (GROUPS, EXPERTS, SLOTS), 0, GROUPS), jax.random.fold_in(key_of[3], 1), 0, GROUPS - 1).astype(jnp.int32)
    slot_row = place_ends(jax.random.randint(key_of[4], (GROUPS, EXPERTS, SLOTS), 0, TOK_DEV), jax.random.fold_in(key_of[4], 1), 0, TOK_DEV - 1).astype(jnp.int32)
    block_count = draw_block_count(jax.random.fold_in(key_of[6], 71), 0)
    return {"hidden": hidden, "down_weight": down_weight, "slot_gate": slot_gate, "slot_owner": slot_owner, "slot_row": slot_row, "block_count": block_count}


def reference(hidden, down_weight, slot_gate, slot_owner, slot_row, block_count):
    column = (jnp.arange(SLOTS) // SEND).astype(jnp.int32)
    within = (jnp.arange(SLOTS) % SEND).astype(jnp.int32)

    def expert_rows(pair):
        rows_in, weight = pair
        return jnp.dot(rows_in, weight, preferred_element_type=jnp.float32)

    def group_step(total, inputs):
        group_hidden, gates, owners, row_index, counts = inputs
        product = lax.map(expert_rows, (group_hidden, down_weight))
        live = (within[None, :] < counts[:, column]).astype(jnp.float32)
        scale = gates * live
        sent = (product * scale[:, :, None]).astype(jnp.bfloat16)
        token = ((owners * N_EP + column[None, :]) * TOK_DEV + row_index).astype(jnp.int32)
        summed = jax.ops.segment_sum(sent.reshape(-1, D).astype(jnp.float32), token.reshape(-1), num_segments=TOKENS)
        rounded = lax.optimization_barrier(summed.astype(jnp.bfloat16))
        return total + rounded.astype(jnp.float32), None

    start = jnp.zeros((TOKENS, D), jnp.float32)
    total, unused = lax.scan(group_step, start, (hidden, slot_gate, slot_owner, slot_row, block_count))
    return total.astype(jnp.bfloat16)
```

```python
import functools

import jax
import jax.numpy as jnp
from jax import lax
from jax.experimental import pallas as pl
from jax.experimental.pallas import tpu as pltpu
from jax.sharding import PartitionSpec as P

TOK_DEV = 32
LANES = 128
VMEM_ROOM = 48 * 1024 * 1024
MESH = pl.DeviceIdType.MESH


def exchange_body(hidden, down_weight, slot_gate, slot_owner, slot_row, block_count):
    columns = lax.axis_size("ep")
    slot_total = hidden.shape[2]
    send = slot_total // columns
    product = jnp.dot(hidden[0, 0], down_weight[0], preferred_element_type=jnp.float32)
    within = jnp.arange(slot_total) % send
    limits = jnp.repeat(block_count[0, 0], send)
    live = (within < limits).astype(jnp.float32)
    scaled = (product * (slot_gate[0, 0] * live)[:, None]).astype(jnp.bfloat16)
    local_index = slot_owner[0, 0] * TOK_DEV + slot_row[0, 0]
    arrived, arrived_index = (
        lax.all_to_all(scaled, "ep", split_axis=0, concat_axis=0, tiled=True),
        lax.all_to_all(local_index, "ep", split_axis=0, concat_axis=0, tiled=True),
    )
    wanted = jnp.arange(lax.axis_size("grp") * TOK_DEV)
    table = (wanted[:, None] == arrived_index[None, :]).astype(jnp.bfloat16)
    return lax.psum_scatter(
        jnp.dot(table, arrived, preferred_element_type=jnp.float32).astype(jnp.bfloat16),
        "grp",
        scatter_dimension=0,
        tiled=True,
    )


def partner(me, n, k):
    if n & (n - 1):
        return lax.rem(me + n - k, n), lax.rem(me + k, n)
    other, bit = 0, 1
    while bit < n:
        mine = lax.rem(me // bit, 2)
        other = other + bit * (1 - mine if k & bit else mine)
        bit *= 2
    return other, other


def kernel(
    groups, columns, send, piece,
    hidden_ref, weight_ref, gate_ref, owner_ref, row_ref, count_ref, out_ref,
    weight, rows_in, meta, outgoing, arrived, places,
    weight_sem, hid_send, hid_recv, meta_send, meta_recv,
    row_send, row_recv, place_send, place_recv,
):
    group, column = lax.axis_index("grp"), lax.axis_index("ep")
    slots, width = hidden_ref.shape[2], weight_ref.shape[2]
    pieces = width // piece
    group_steps = list(range(1, groups))
    column_steps = sorted(range(1, columns), key=lambda k: (k % 2, -k)) if columns > 1 else []

    def weight_copy(j):
        cols = pl.ds(j * piece, piece)
        return pltpu.make_async_copy(
            weight_ref.at[0, :, cols], weight.at[:, cols], weight_sem.at[j]
        )

    for j in range(pieces):
        weight_copy(j).start()

    barrier = pltpu.get_barrier_semaphore()
    for k in group_steps:
        pl.semaphore_signal(
            barrier, inc=1, device_id=(partner(group, groups, k)[0], column), device_id_type=MESH
        )
    for k in column_steps:
        pl.semaphore_signal(
            barrier, inc=1, device_id=(group, partner(column, columns, k)[0]), device_id_type=MESH
        )

    lane = lax.broadcasted_iota(jnp.int32, (1, slots), 1)
    limit = jnp.zeros((1, slots), jnp.int32)
    for q in range(columns):
        limit = jnp.where(lane // send == q, count_ref[0, :, q:q + 1], limit)
    scale = jnp.where(lane % send < limit, gate_ref[0], 0.0)
    meta[0] = jnp.zeros(meta.shape[1:], jnp.float32)
    meta[0, 0, :, :slots] = scale
    meta[0, 1, :, :slots] = (owner_ref[0] * TOK_DEV + row_ref[0]).astype(jnp.float32)
    rows_in[0] = hidden_ref[0, 0]

    pl.semaphore_wait(barrier, groups + columns - 2)

    def hidden_copy(k):
        return pltpu.make_async_remote_copy(
            src_ref=hidden_ref.at[0, 0], dst_ref=rows_in.at[k],
            send_sem=hid_send.at[k], recv_sem=hid_recv.at[k],
            device_id=(partner(group, groups, k)[0], column), device_id_type=MESH,
        )

    def meta_copy(k):
        return pltpu.make_async_remote_copy(
            src_ref=meta.at[0], dst_ref=meta.at[k],
            send_sem=meta_send.at[k], recv_sem=meta_recv.at[k],
            device_id=(partner(group, groups, k)[0], column), device_id_type=MESH,
        )

    def row_copy(k, m):
        to = partner(column, columns, m)[0]
        return pltpu.make_async_remote_copy(
            src_ref=outgoing.at[k, to], dst_ref=arrived.at[k, column],
            send_sem=row_send.at[k, m], recv_sem=row_recv.at[k, m],
            device_id=(group, to), device_id_type=MESH,
        )

    def place_copy(k, m):
        return pltpu.make_async_remote_copy(
            src_ref=meta.at[k, 1], dst_ref=places.at[k, column],
            send_sem=place_send.at[k, m], recv_sem=place_recv.at[k, m],
            device_id=(group, partner(column, columns, m)[0]), device_id_type=MESH,
        )

    for k in group_steps:
        meta_copy(k).start()
        hidden_copy(k).start()

    eye = lax.broadcasted_iota(jnp.int32, (slots, slots), 0) == lax.broadcasted_iota(
        jnp.int32, (slots, slots), 1
    )
    for k in range(groups):
        if k:
            meta_copy(k).wait_recv()
            hidden_copy(k).wait_recv()
        for m in column_steps:
            place_copy(k, m).start()
        places[k, column] = meta[k, 1]
        factor = jnp.sum(jnp.where(eye, meta[k, 0, :, :slots], 0.0), axis=1, keepdims=True)
        for j in range(pieces):
            if k == 0:
                weight_copy(j).wait()
            cols = slice(j * piece, (j + 1) * piece)
            product = jnp.dot(rows_in[k], weight[:, cols], preferred_element_type=jnp.float32)
            scaled = product * factor
            for q in range(columns):
                outgoing[k, q, :, cols] = scaled[q * send:(q + 1) * send].astype(jnp.bfloat16)
        for m in column_steps:
            row_copy(k, m).start()
        arrived[k, column] = outgoing[k, column]

    total = columns * send
    picked = lax.broadcasted_iota(jnp.int32, (meta.shape[3], total), 0) == (
        column * send + lax.broadcasted_iota(jnp.int32, (meta.shape[3], total), 1) % send
    )
    picked = picked.astype(jnp.float32)
    mine = lax.broadcasted_iota(jnp.int32, (columns, total), 0) == (
        lax.broadcasted_iota(jnp.int32, (columns, total), 1) // send
    )
    wanted = (
        group * TOK_DEV + lax.broadcasted_iota(jnp.int32, (TOK_DEV, total), 0)
    ).astype(jnp.float32)
    tables = []
    for k in range(groups):
        for m in column_steps:
            place_copy(k, m).wait_recv()
        index = jnp.dot(
            places[k, :, 0], picked,
            precision=lax.Precision.HIGHEST, preferred_element_type=jnp.float32,
        )
        index = jnp.sum(jnp.where(mine, index, 0.0), axis=0, keepdims=True)
        tables.append((wanted == index).astype(jnp.bfloat16))
    for k in range(groups):
        for m in column_steps:
            row_copy(k, m).wait_recv()
    for j in range(pieces):
        cols = slice(j * piece, (j + 1) * piece)
        total_rows = jnp.zeros((TOK_DEV, piece), jnp.float32)
        for k in range(groups):
            block = jnp.concatenate([arrived[k, e, :, cols] for e in range(columns)], axis=0)
            total_rows += jnp.dot(tables[k], block, preferred_element_type=jnp.float32)
        out_ref[:, cols] = total_rows.astype(out_ref.dtype)

    for k in group_steps:
        meta_copy(k).wait_send()
        hidden_copy(k).wait_send()
    for k in range(groups):
        for m in column_steps:
            place_copy(k, m).wait_send()
            row_copy(k, m).wait_send()


def kernel_body(hidden, down_weight, slot_gate, slot_owner, slot_row, block_count):
    groups, columns = lax.axis_size("grp"), lax.axis_size("ep")
    slots, depth = hidden.shape[2:]
    width = down_weight.shape[2]
    send = slots // columns
    lanes = -(-slots // LANES) * LANES
    piece = 1024 if width % 1024 == 0 else width
    vmem = pl.BlockSpec(memory_space=pltpu.VMEM)
    dma = pltpu.SemaphoreType.DMA
    return pl.pallas_call(
        functools.partial(kernel, groups, columns, send, piece),
        out_shape=jax.ShapeDtypeStruct((TOK_DEV, width), jnp.bfloat16),
        in_specs=[vmem, pl.BlockSpec(memory_space=pl.ANY), vmem, vmem, vmem, vmem],
        out_specs=vmem,
        scratch_shapes=[
            pltpu.VMEM((depth, width), jnp.bfloat16),
            pltpu.VMEM((groups, slots, depth), jnp.bfloat16),
            pltpu.VMEM((groups, 2, 1, lanes), jnp.float32),
            pltpu.VMEM((groups, columns, send, width), jnp.bfloat16),
            pltpu.VMEM((groups, columns, send, width), jnp.bfloat16),
            pltpu.VMEM((groups, columns, 1, lanes), jnp.float32),
            dma((width // piece,)),
            dma((groups,)), dma((groups,)), dma((groups,)), dma((groups,)),
            dma((groups, columns)), dma((groups, columns)),
            dma((groups, columns)), dma((groups, columns)),
        ],
        compiler_params=pltpu.CompilerParams(
            collective_id=0, has_side_effects=True, vmem_limit_bytes=56 * 1024 * 1024
        ),
    )(hidden, down_weight, slot_gate, slot_owner, slot_row, block_count)


def body(hidden, down_weight, *slot_data):
    groups, columns = lax.axis_size("grp"), lax.axis_size("ep")
    slots, depth = hidden.shape[2:]
    width = down_weight.shape[2]
    held = 2 * (depth * width + groups * slots * (depth + 2 * width))
    chosen = kernel_body if held <= VMEM_ROOM else exchange_body
    return chosen(hidden, down_weight, *slot_data)


def solution(mesh):
    in_specs = (
        P("grp", "ep", None, None),
        P("ep", None, None),
        P("grp", "ep", None),
        P("grp", "ep", None),
        P("grp", "ep", None),
        P("grp", "ep", None),
    )
    out_specs = P(("grp", "ep"), None)
    return jax.shard_map(body, mesh=mesh, in_specs=in_specs, out_specs=out_specs, check_vma=False)
```

```python
import functools

import jax
import jax.numpy as jnp
from jax import lax
from jax.experimental import pallas as pl
from jax.experimental.pallas import tpu as pltpu
from jax.sharding import PartitionSpec as P

TOK_DEV = 32
LANES = 128
VMEM_ROOM = 48 * 1024 * 1024
MESH = pl.DeviceIdType.MESH


def exchange_body(hidden, down_weight, slot_gate, slot_owner, slot_row, block_count):
    columns = lax.axis_size("ep")
    slot_total = hidden.shape[2]
    send = slot_total // columns
    product = jnp.dot(hidden[0, 0], down_weight[0], preferred_element_type=jnp.float32)
    within = jnp.arange(slot_total) % send
    limits = jnp.repeat(block_count[0, 0], send)
    live = (within < limits).astype(jnp.float32)
    scaled = (product * (slot_gate[0, 0] * live)[:, None]).astype(jnp.bfloat16)
    local_index = slot_owner[0, 0] * TOK_DEV + slot_row[0, 0]
    arrived, arrived_index = (
        lax.all_to_all(scaled, "ep", split_axis=0, concat_axis=0, tiled=True),
        lax.all_to_all(local_index, "ep", split_axis=0, concat_axis=0, tiled=True),
    )
    wanted = jnp.arange(lax.axis_size("grp") * TOK_DEV)
    table = (wanted[:, None] == arrived_index[None, :]).astype(jnp.bfloat16)
    return lax.psum_scatter(
        jnp.dot(table, arrived, preferred_element_type=jnp.float32).astype(jnp.bfloat16),
        "grp",
        scatter_dimension=0,
        tiled=True,
    )


def partner(me, n, k):
    if n & (n - 1):
        return lax.rem(me + n - k, n), lax.rem(me + k, n)
    other, bit = 0, 1
    while bit < n:
        mine = lax.rem(me // bit, 2)
        other = other + bit * (1 - mine if k & bit else mine)
        bit *= 2
    return other, other


def kernel(
    groups, columns, send, piece,
    hidden_ref, weight_ref, gate_ref, owner_ref, row_ref, count_ref, out_ref,
    gate, owner, row, count, result, weight, rows_in, meta, outgoing, arrived, places,
    load_sem, store_sem, weight_sem, hid_send, hid_recv, meta_send, meta_recv,
    row_send, row_recv, place_send, place_recv,
):
    group, column = lax.axis_index("grp"), lax.axis_index("ep")
    slots, width = hidden_ref.shape[2], weight_ref.shape[2]
    pieces = width // piece
    group_steps = list(range(1, groups))
    column_steps = sorted(range(1, columns), key=lambda k: (k % 2, -k)) if columns > 1 else []

    def weight_copy(j):
        cols = pl.ds(j * piece, piece)
        return pltpu.make_async_copy(
            weight_ref.at[0, :, cols], weight.at[:, cols], weight_sem.at[j]
        )

    def result_copy(j):
        cols = pl.ds(j * piece, piece)
        return pltpu.make_async_copy(result.at[:, cols], out_ref.at[:, cols], store_sem.at[j])

    barrier = pltpu.get_barrier_semaphore()
    for k in group_steps:
        pl.semaphore_signal(
            barrier, inc=1, device_id=(partner(group, groups, k)[0], column), device_id_type=MESH
        )
    for k in column_steps:
        pl.semaphore_signal(
            barrier, inc=1, device_id=(group, partner(column, columns, k)[0]), device_id_type=MESH
        )

    loads = [
        pltpu.make_async_copy(gate_ref.at[0], gate, load_sem.at[0]),
        pltpu.make_async_copy(owner_ref.at[0], owner, load_sem.at[1]),
        pltpu.make_async_copy(row_ref.at[0], row, load_sem.at[2]),
        pltpu.make_async_copy(count_ref.at[0], count, load_sem.at[3]),
        pltpu.make_async_copy(hidden_ref.at[0, 0], rows_in.at[0], load_sem.at[4]),
    ]
    for load in loads:
        load.start()
    for j in range(pieces):
        weight_copy(j).start()

    for load in loads:
        load.wait()
    lane = lax.broadcasted_iota(jnp.int32, (1, slots), 1)
    limit = jnp.zeros((1, slots), jnp.int32)
    for q in range(columns):
        limit = jnp.where(lane // send == q, count[:, q:q + 1], limit)
    scale = jnp.where(lane % send < limit, gate[...], 0.0)
    meta[0] = jnp.zeros(meta.shape[1:], jnp.float32)
    meta[0, 0, :, :slots] = scale
    meta[0, 1, :, :slots] = (owner[...] * TOK_DEV + row[...]).astype(jnp.float32)

    pl.semaphore_wait(barrier, groups + columns - 2)

    def hidden_copy(k):
        return pltpu.make_async_remote_copy(
            src_ref=rows_in.at[0], dst_ref=rows_in.at[k],
            send_sem=hid_send.at[k], recv_sem=hid_recv.at[k],
            device_id=(partner(group, groups, k)[0], column), device_id_type=MESH,
        )

    def meta_copy(k):
        return pltpu.make_async_remote_copy(
            src_ref=meta.at[0], dst_ref=meta.at[k],
            send_sem=meta_send.at[k], recv_sem=meta_recv.at[k],
            device_id=(partner(group, groups, k)[0], column), device_id_type=MESH,
        )

    def row_copy(k, m):
        to = partner(column, columns, m)[0]
        return pltpu.make_async_remote_copy(
            src_ref=outgoing.at[k, to], dst_ref=arrived.at[k, column],
            send_sem=row_send.at[k, m], recv_sem=row_recv.at[k, m],
            device_id=(group, to), device_id_type=MESH,
        )

    def place_copy(k, m):
        return pltpu.make_async_remote_copy(
            src_ref=meta.at[k, 1], dst_ref=places.at[k, column],
            send_sem=place_send.at[k, m], recv_sem=place_recv.at[k, m],
            device_id=(group, partner(column, columns, m)[0]), device_id_type=MESH,
        )

    for k in group_steps:
        meta_copy(k).start()
        hidden_copy(k).start()

    eye = lax.broadcasted_iota(jnp.int32, (slots, slots), 0) == lax.broadcasted_iota(
        jnp.int32, (slots, slots), 1
    )
    for k in range(groups):
        if k:
            meta_copy(k).wait_recv()
            hidden_copy(k).wait_recv()
        for m in column_steps:
            place_copy(k, m).start()
        places[k, column] = meta[k, 1]
        factor = jnp.sum(jnp.where(eye, meta[k, 0, :, :slots], 0.0), axis=1, keepdims=True)
        for j in range(pieces):
            if k == 0:
                weight_copy(j).wait()
            cols = slice(j * piece, (j + 1) * piece)
            product = jnp.dot(rows_in[k], weight[:, cols], preferred_element_type=jnp.float32)
            scaled = product * factor
            for q in range(columns):
                outgoing[k, q, :, cols] = scaled[q * send:(q + 1) * send].astype(jnp.bfloat16)
        for m in column_steps:
            row_copy(k, m).start()
        arrived[k, column] = outgoing[k, column]

    total = columns * send
    picked = lax.broadcasted_iota(jnp.int32, (meta.shape[3], total), 0) == (
        column * send + lax.broadcasted_iota(jnp.int32, (meta.shape[3], total), 1) % send
    )
    picked = picked.astype(jnp.float32)
    mine = lax.broadcasted_iota(jnp.int32, (columns, total), 0) == (
        lax.broadcasted_iota(jnp.int32, (columns, total), 1) // send
    )
    wanted = (
        group * TOK_DEV + lax.broadcasted_iota(jnp.int32, (TOK_DEV, total), 0)
    ).astype(jnp.float32)
    tables = []
    for k in range(groups):
        for m in column_steps:
            place_copy(k, m).wait_recv()
        index = jnp.dot(
            places[k, :, 0], picked,
            precision=lax.Precision.HIGHEST, preferred_element_type=jnp.float32,
        )
        index = jnp.sum(jnp.where(mine, index, 0.0), axis=0, keepdims=True)
        tables.append((wanted == index).astype(jnp.bfloat16))
    for k in range(groups):
        for m in column_steps:
            row_copy(k, m).wait_recv()
    for j in range(pieces):
        cols = slice(j * piece, (j + 1) * piece)
        total_rows = jnp.zeros((TOK_DEV, piece), jnp.float32)
        for k in range(groups):
            block = jnp.concatenate([arrived[k, e, :, cols] for e in range(columns)], axis=0)
            total_rows += jnp.dot(tables[k], block, preferred_element_type=jnp.float32)
        result[:, cols] = total_rows.astype(out_ref.dtype)
        result_copy(j).start()

    for k in group_steps:
        meta_copy(k).wait_send()
        hidden_copy(k).wait_send()
    for k in range(groups):
        for m in column_steps:
            place_copy(k, m).wait_send()
            row_copy(k, m).wait_send()
    for j in range(pieces):
        result_copy(j).wait()


def kernel_body(hidden, down_weight, slot_gate, slot_owner, slot_row, block_count):
    groups, columns = lax.axis_size("grp"), lax.axis_size("ep")
    slots, depth = hidden.shape[2:]
    width = down_weight.shape[2]
    send = slots // columns
    lanes = -(-slots // LANES) * LANES
    piece = 1024 if width % 1024 == 0 else width
    hbm = pl.BlockSpec(memory_space=pltpu.HBM)
    dma = pltpu.SemaphoreType.DMA
    return pl.pallas_call(
        functools.partial(kernel, groups, columns, send, piece),
        out_shape=jax.ShapeDtypeStruct((TOK_DEV, width), jnp.bfloat16),
        in_specs=[hbm] * 6,
        out_specs=hbm,
        scratch_shapes=[
            pltpu.VMEM((1, slots), jnp.float32),
            pltpu.VMEM((1, slots), jnp.int32),
            pltpu.VMEM((1, slots), jnp.int32),
            pltpu.VMEM((1, columns), jnp.int32),
            pltpu.VMEM((TOK_DEV, width), jnp.bfloat16),
            pltpu.VMEM((depth, width), jnp.bfloat16),
            pltpu.VMEM((groups, slots, depth), jnp.bfloat16),
            pltpu.VMEM((groups, 2, 1, lanes), jnp.float32),
            pltpu.VMEM((groups, columns, send, width), jnp.bfloat16),
            pltpu.VMEM((groups, columns, send, width), jnp.bfloat16),
            pltpu.VMEM((groups, columns, 1, lanes), jnp.float32),
            dma((5,)), dma((width // piece,)), dma((width // piece,)),
            dma((groups,)), dma((groups,)), dma((groups,)), dma((groups,)),
            dma((groups, columns)), dma((groups, columns)),
            dma((groups, columns)), dma((groups, columns)),
        ],
        compiler_params=pltpu.CompilerParams(
            collective_id=0, has_side_effects=True, vmem_limit_bytes=56 * 1024 * 1024
        ),
    )(hidden, down_weight, slot_gate, slot_owner, slot_row, block_count)


def body(hidden, down_weight, *slot_data):
    groups, columns = lax.axis_size("grp"), lax.axis_size("ep")
    slots, depth = hidden.shape[2:]
    width = down_weight.shape[2]
    held = 2 * (depth * width + groups * slots * (depth + 2 * width))
    chosen = kernel_body if held <= VMEM_ROOM else exchange_body
    return chosen(hidden, down_weight, *slot_data)


def solution(mesh):
    in_specs = (
        P("grp", "ep", None, None),
        P("ep", None, None),
        P("grp", "ep", None),
        P("grp", "ep", None),
        P("grp", "ep", None),
        P("grp", "ep", None),
    )
    out_specs = P(("grp", "ep"), None)
    return jax.shard_map(body, mesh=mesh, in_specs=in_specs, out_specs=out_specs, check_vma=False)
```

```python
import functools

import jax
import jax.numpy as jnp
from jax import lax
from jax.experimental import pallas as pl
from jax.experimental.pallas import tpu as pltpu
from jax.sharding import PartitionSpec as P

TOK_DEV = 32
LANES = 128
VMEM_ROOM = 48 * 1024 * 1024
MESH = pl.DeviceIdType.MESH


def exchange_body(hidden, down_weight, slot_gate, slot_owner, slot_row, block_count):
    columns = lax.axis_size("ep")
    slot_total = hidden.shape[2]
    send = slot_total // columns
    product = jnp.dot(hidden[0, 0], down_weight[0], preferred_element_type=jnp.float32)
    within = jnp.arange(slot_total) % send
    limits = jnp.repeat(block_count[0, 0], send)
    live = (within < limits).astype(jnp.float32)
    scaled = (product * (slot_gate[0, 0] * live)[:, None]).astype(jnp.bfloat16)
    local_index = slot_owner[0, 0] * TOK_DEV + slot_row[0, 0]
    arrived, arrived_index = (
        lax.all_to_all(scaled, "ep", split_axis=0, concat_axis=0, tiled=True),
        lax.all_to_all(local_index, "ep", split_axis=0, concat_axis=0, tiled=True),
    )
    wanted = jnp.arange(lax.axis_size("grp") * TOK_DEV)
    table = (wanted[:, None] == arrived_index[None, :]).astype(jnp.bfloat16)
    return lax.psum_scatter(
        jnp.dot(table, arrived, preferred_element_type=jnp.float32).astype(jnp.bfloat16),
        "grp",
        scatter_dimension=0,
        tiled=True,
    )


def partner(me, n, k):
    if n & (n - 1):
        return lax.rem(me + n - k, n), lax.rem(me + k, n)
    other, bit = 0, 1
    while bit < n:
        mine = lax.rem(me // bit, 2)
        other = other + bit * (1 - mine if k & bit else mine)
        bit *= 2
    return other, other


def kernel(
    groups, columns, send, piece,
    hidden_ref, weight_ref, gate_ref, owner_ref, row_ref, count_ref, out_ref,
    gate, owner, row, count, sums, result, weight, rows_in, meta, outgoing, arrived, places,
    load_sem, store_sem, weight_sem, hid_send, hid_recv, meta_send, meta_recv,
    row_send, row_recv, place_send, place_recv,
):
    group, column = lax.axis_index("grp"), lax.axis_index("ep")
    slots, width = hidden_ref.shape[2], weight_ref.shape[2]
    pieces = width // piece
    batches = [2 if k == 0 and pieces % 2 == 0 else pieces for k in range(groups)]
    group_steps = list(range(1, groups))
    column_steps = sorted(range(1, columns), key=lambda k: (k % 2, -k)) if columns > 1 else []

    def weight_copy(j):
        cols = pl.ds(j * piece, piece)
        return pltpu.make_async_copy(
            weight_ref.at[0, :, cols], weight.at[:, cols], weight_sem.at[j]
        )

    def result_copy(j):
        cols = pl.ds(j * piece, piece)
        return pltpu.make_async_copy(result.at[:, cols], out_ref.at[:, cols], store_sem.at[j])

    barrier = pltpu.get_barrier_semaphore()
    for k in group_steps:
        pl.semaphore_signal(
            barrier, inc=1, device_id=(partner(group, groups, k)[0], column), device_id_type=MESH
        )
    for k in column_steps:
        pl.semaphore_signal(
            barrier, inc=1, device_id=(group, partner(column, columns, k)[0]), device_id_type=MESH
        )

    loads = [
        pltpu.make_async_copy(gate_ref.at[0], gate, load_sem.at[0]),
        pltpu.make_async_copy(owner_ref.at[0], owner, load_sem.at[1]),
        pltpu.make_async_copy(row_ref.at[0], row, load_sem.at[2]),
        pltpu.make_async_copy(count_ref.at[0], count, load_sem.at[3]),
        pltpu.make_async_copy(hidden_ref.at[0, 0], rows_in.at[0], load_sem.at[4]),
    ]
    for load in loads:
        load.start()
    for j in range(pieces):
        weight_copy(j).start()

    for load in loads:
        load.wait()
    lane = lax.broadcasted_iota(jnp.int32, (1, slots), 1)
    limit = jnp.zeros((1, slots), jnp.int32)
    for q in range(columns):
        limit = jnp.where(lane // send == q, count[:, q:q + 1], limit)
    scale = jnp.where(lane % send < limit, gate[...], 0.0)
    meta[0] = jnp.zeros(meta.shape[1:], jnp.float32)
    meta[0, 0, :, :slots] = scale
    meta[0, 1, :, :slots] = (owner[...] * TOK_DEV + row[...]).astype(jnp.float32)

    pl.semaphore_wait(barrier, groups + columns - 2)

    def hidden_copy(k):
        return pltpu.make_async_remote_copy(
            src_ref=rows_in.at[0], dst_ref=rows_in.at[k],
            send_sem=hid_send.at[k], recv_sem=hid_recv.at[k],
            device_id=(partner(group, groups, k)[0], column), device_id_type=MESH,
        )

    def meta_copy(k):
        return pltpu.make_async_remote_copy(
            src_ref=meta.at[0], dst_ref=meta.at[k],
            send_sem=meta_send.at[k], recv_sem=meta_recv.at[k],
            device_id=(partner(group, groups, k)[0], column), device_id_type=MESH,
        )

    def row_copy(k, m, j):
        to = partner(column, columns, m)[0]
        cols = pl.ds(j * piece, batches[k] * piece)
        return pltpu.make_async_remote_copy(
            src_ref=outgoing.at[k, to, :, cols], dst_ref=arrived.at[k, column, :, cols],
            send_sem=row_send.at[k], recv_sem=row_recv.at[k],
            device_id=(group, to), device_id_type=MESH,
        )

    def place_copy(k, m):
        return pltpu.make_async_remote_copy(
            src_ref=meta.at[k, 1], dst_ref=places.at[k, column],
            send_sem=place_send.at[k], recv_sem=place_recv.at[k],
            device_id=(group, partner(column, columns, m)[0]), device_id_type=MESH,
        )

    def all_rows(k):
        return pltpu.make_async_remote_copy(
            src_ref=outgoing.at[k, pl.ds(0, columns - 1)],
            dst_ref=arrived.at[k, pl.ds(0, columns - 1)],
            send_sem=row_send.at[k], recv_sem=row_recv.at[k],
            device_id=(group, partner(column, columns, 1)[0]), device_id_type=MESH,
        )

    def all_places(k):
        return pltpu.make_async_remote_copy(
            src_ref=places.at[k, pl.ds(0, columns - 1)],
            dst_ref=places.at[k, pl.ds(0, columns - 1)],
            send_sem=place_send.at[k], recv_sem=place_recv.at[k],
            device_id=(group, partner(column, columns, 1)[0]), device_id_type=MESH,
        )

    for k in group_steps:
        meta_copy(k).start()
        hidden_copy(k).start()

    eye = lax.broadcasted_iota(jnp.int32, (slots, slots), 0) == lax.broadcasted_iota(
        jnp.int32, (slots, slots), 1
    )
    for k in range(groups):
        if k:
            meta_copy(k).wait_recv()
            hidden_copy(k).wait_recv()
        for m in column_steps:
            place_copy(k, m).start()
        places[k, column] = meta[k, 1]
        factor = jnp.sum(jnp.where(eye, meta[k, 0, :, :slots], 0.0), axis=1, keepdims=True)
        for j in range(pieces):
            if k == 0:
                weight_copy(j).wait()
            cols = slice(j * piece, (j + 1) * piece)
            product = jnp.dot(rows_in[k], weight[:, cols], preferred_element_type=jnp.float32)
            scaled = product * factor
            for q in range(columns):
                outgoing[k, q, :, cols] = scaled[q * send:(q + 1) * send].astype(jnp.bfloat16)
            if (j + 1) % batches[k] == 0:
                for m in column_steps:
                    row_copy(k, m, j + 1 - batches[k]).start()
        arrived[k, column] = outgoing[k, column]

    total = columns * send
    picked = lax.broadcasted_iota(jnp.int32, (meta.shape[3], total), 0) == (
        column * send + lax.broadcasted_iota(jnp.int32, (meta.shape[3], total), 1) % send
    )
    picked = picked.astype(jnp.float32)
    mine = lax.broadcasted_iota(jnp.int32, (columns, total), 0) == (
        lax.broadcasted_iota(jnp.int32, (columns, total), 1) // send
    )
    wanted = (
        group * TOK_DEV + lax.broadcasted_iota(jnp.int32, (TOK_DEV, total), 0)
    ).astype(jnp.float32)
    tables = []
    for k in range(groups):
        if column_steps:
            all_places(k).wait_recv()
        index = jnp.dot(
            places[k, :, 0], picked,
            precision=lax.Precision.HIGHEST, preferred_element_type=jnp.float32,
        )
        index = jnp.sum(jnp.where(mine, index, 0.0), axis=0, keepdims=True)
        tables.append((wanted == index).astype(jnp.bfloat16))
    for k in range(groups):
        if column_steps:
            all_rows(k).wait_recv()
        for j in range(pieces):
            cols = slice(j * piece, (j + 1) * piece)
            block = jnp.concatenate([arrived[k, e, :, cols] for e in range(columns)], axis=0)
            rows = jnp.dot(tables[k], block, preferred_element_type=jnp.float32)
            if k:
                rows = sums[:, cols] + rows
            if k < groups - 1:
                sums[:, cols] = rows
            else:
                result[:, cols] = rows.astype(out_ref.dtype)
                result_copy(j).start()

    for k in group_steps:
        meta_copy(k).wait_send()
        hidden_copy(k).wait_send()
    for k in range(groups):
        if column_steps:
            all_places(k).wait_send()
            all_rows(k).wait_send()
    for j in range(pieces):
        result_copy(j).wait()


def kernel_body(hidden, down_weight, slot_gate, slot_owner, slot_row, block_count):
    groups, columns = lax.axis_size("grp"), lax.axis_size("ep")
    slots, depth = hidden.shape[2:]
    width = down_weight.shape[2]
    send = slots // columns
    lanes = -(-slots // LANES) * LANES
    piece = 1024 if width % 1024 == 0 else width
    hbm = pl.BlockSpec(memory_space=pltpu.HBM)
    dma = pltpu.SemaphoreType.DMA
    return pl.pallas_call(
        functools.partial(kernel, groups, columns, send, piece),
        out_shape=jax.ShapeDtypeStruct((TOK_DEV, width), jnp.bfloat16),
        in_specs=[hbm] * 6,
        out_specs=hbm,
        scratch_shapes=[
            pltpu.VMEM((1, slots), jnp.float32),
            pltpu.VMEM((1, slots), jnp.int32),
            pltpu.VMEM((1, slots), jnp.int32),
            pltpu.VMEM((1, columns), jnp.int32),
            pltpu.VMEM((TOK_DEV, width), jnp.float32),
            pltpu.VMEM((TOK_DEV, width), jnp.bfloat16),
            pltpu.VMEM((depth, width), jnp.bfloat16),
            pltpu.VMEM((groups, slots, depth), jnp.bfloat16),
            pltpu.VMEM((groups, 2, 1, lanes), jnp.float32),
            pltpu.VMEM((groups, columns, send, width), jnp.bfloat16),
            pltpu.VMEM((groups, columns, send, width), jnp.bfloat16),
            pltpu.VMEM((groups, columns, 1, lanes), jnp.float32),
            dma((5,)), dma((width // piece,)), dma((width // piece,)),
            dma((groups,)), dma((groups,)), dma((groups,)), dma((groups,)),
            dma((groups,)), dma((groups,)), dma((groups,)), dma((groups,)),
        ],
        compiler_params=pltpu.CompilerParams(
            collective_id=0, has_side_effects=True, vmem_limit_bytes=56 * 1024 * 1024
        ),
    )(hidden, down_weight, slot_gate, slot_owner, slot_row, block_count)


def body(hidden, down_weight, *slot_data):
    groups, columns = lax.axis_size("grp"), lax.axis_size("ep")
    slots, depth = hidden.shape[2:]
    width = down_weight.shape[2]
    held = 2 * (depth * width + groups * slots * (depth + 2 * width))
    chosen = kernel_body if held <= VMEM_ROOM else exchange_body
    return chosen(hidden, down_weight, *slot_data)


def solution(mesh):
    in_specs = (
        P("grp", "ep", None, None),
        P("ep", None, None),
        P("grp", "ep", None),
        P("grp", "ep", None),
        P("grp", "ep", None),
        P("grp", "ep", None),
    )
    out_specs = P(("grp", "ep"), None)
    return jax.shard_map(body, mesh=mesh, in_specs=in_specs, out_specs=out_specs, check_vma=False)
```
